32 devices in a mesh: dp: 8 (over z, y), seq: 4 (over x, core).
Axes of the slice: x: 2, y: 2, z: 4, core: 2. Of those that a mesh axis runs over, the one named last changes fastest.
Arguments:
- byte_states: bfloat16 [8, 1024, 1024], P('dp', 'seq'), may hold values from -6 to 6
- kv_weight: bfloat16 [1024, 1024], P('dp'), may hold values from -0.1875 to 0.1875
- patch_query: bfloat16 [8, 256, 512], P('dp', 'seq'), may hold values from -96 to 96
- out_grad: bfloat16 [8, 256, 512], P('dp', 'seq'), may hold values from -3 to 3
- patch_start: int32 [8, 4, 64], P('dp'), may hold values from 0 to 256, as said below
- patch_count: int32 [8, 4], P('dp'), may hold values from 16 to 64, as said below
Outputs:
- byte_grad: bfloat16 [8, 1024, 1024], P('dp', 'seq')
- query_grad: bfloat16 [8, 256, 512], P('dp', 'seq')
- kv_grad: float32 [1024, 1024], P('dp', 'seq')
The draws below stay inside these ranges and needn't reach their ends.
Inputs may be any that keep to these rules, and one draw needn't show every extreme that they name: `patch_start`: within a shard the live starts rise strictly; the first start is below 64 and equals 63 in some shard; slots from patch_count on hold 256. `patch_count`: some shard holds 64 patches.
All inputs are finite; a program needn't handle non-finite values.
Results may differ from the reference program's by a relative error of at most 0.03.
Values may be sent and summed in bfloat16 or wider, within the bound.
A program may use at most 64 MiB of HBM per device.

```python
import math
import jax
import jax.numpy as jnp
from jax import lax

D = 1024
HEADS = 8
HD = 64
HK = 512
BYTES_DEV = 256
PSLOT = 64
PMIN = 16
REACH = 64
SEQS = 8
LENGTH = 1024
N_SEQ = 4


def patch_layout(key):
    base = jax.random.fold_in(key, 7)
    key_list = jax.random.split(base, 4)
    seq_index = jnp.arange(SEQS, dtype=jnp.int32)[:, None]
    shard_index = jnp.arange(N_SEQ, dtype=jnp.int32)[None, :]
    ranking = seq_index * (N_SEQ - 1) + shard_index * (SEQS - 1)
    highest = 2 * (SEQS - 1) * (N_SEQ - 1)
    level = PMIN + (PSLOT - PMIN) * ranking // highest
    jitter = jax.random.randint(key_list[0], (SEQS, N_SEQ), 0, 4)
    counts = jnp.maximum(level - jitter, PMIN)
    counts = jnp.where(ranking == highest, PSLOT, counts)
    firsts = jax.random.randint(key_list[1], (SEQS, N_SEQ), 0, REACH)
    chosen_cell = jax.random.randint(key_list[2], (), 0, SEQS * N_SEQ)
    flat_index = seq_index * N_SEQ + shard_index
    firsts = jnp.where(flat_index == chosen_cell, REACH - 1, firsts)
    positions = jnp.arange(BYTES_DEV, dtype=jnp.int32)
    priority = jax.random.randint(key_list[3], (SEQS, N_SEQ, BYTES_DEV), 0, 1 << 20) * BYTES_DEV + positions
    priority = jnp.where(positions[None, None, :] <= firsts[..., None], -1, priority)
    ignored, picked = lax.top_k(priority, PSLOT - 1)
    slot_ids = jnp.arange(PSLOT - 1, dtype=jnp.int32)
    picked = jnp.where(slot_ids[None, None, :] < counts[..., None] - 1, picked, BYTES_DEV)
    picked = jnp.sort(picked, axis=-1)
    starts = jnp.concatenate([firsts[..., None], picked], -1)
    return (starts.astype(jnp.int32), counts.astype(jnp.int32))


def draw_patch_start(key, part):
    return patch_layout(key)[0]


def draw_patch_count(key, part):
    return patch_layout(key)[1]


def draw_patch_query(key, part):
    base = jax.random.fold_in(key, 11)
    key_list = jax.random.split(base, 1)
    values = jnp.clip(jax.random.normal(key_list[0], (SEQS, N_SEQ * PSLOT, HEADS * HD), jnp.float32), -6.0, 6.0)
    return values.astype(jnp.bfloat16)


def level_of(rng, shape, pieces, least, high):
    level = 1.0
    for dim, blocks in pieces:
        heights = jax.random.uniform(jax.random.fold_in(jax.random.fold_in(rng, 6), dim), (blocks,), jnp.float32, least / len(pieces), high / len(pieces))
        level = level * jnp.repeat(jnp.exp(heights), shape[dim] // blocks).reshape((-1,) + (1,) * (len(shape) - 1 - dim))
    return level


def centred(stream_key, extent, deviation, limit, pieces=(), held_as=jnp.bfloat16):
    result = jax.random.normal(stream_key, extent, jnp.float32) * deviation
    if len(pieces) > 0:
        result = level_of(stream_key, extent, pieces, -0.22, 0.18) * result
    return jnp.clip(result, min=-limit, max=limit).astype(held_as)


def setup_inputs(seed: int = 0) -> dict:
    key_of = jax.random.split(jax.random.key(seed), 7)
    return {
        "byte_states": centred(key_of[0], (SEQS, LENGTH, D), 1.0, 6.0, ((0, 8), (1, 4))),
        "kv_weight": centred(key_of[1], (D, 2 * HK), D ** -0.5, 0.1875, ((0, 8),)),
        "patch_query": draw_patch_query(jax.random.fold_in(key_of[6], 71), 0),
        "out_grad": centred(key_of[3], (SEQS, N_SEQ * PSLOT, HK), 0.5, 3.0, ((0, 8), (1, 4))),
        "patch_start": draw_patch_start(jax.random.fold_in(key_of[6], 71), 0),
        "patch_count": draw_patch_count(jax.random.fold_in(key_of[6], 71), 0),
    }


def one_sequence(weight, states, queries, grads_out, starts, counts, loss_scale):
    length = BYTES_DEV * N_SEQ
    patches = N_SEQ * PSLOT
    key_width = HEADS * HD
    attn_scale = 1.0 / math.sqrt(HD)
    slot_ids = jnp.arange(PSLOT, dtype=jnp.int32)
    live_slots = slot_ids[None, :] < counts[:, None]
    global_start = jnp.arange(N_SEQ, dtype=jnp.int32)[:, None] * BYTES_DEV + starts
    global_start = jnp.where(live_slots, global_start, 2 * length).reshape(patches).astype(jnp.int32)
    start_marks = jnp.full((length,), -1, jnp.int32).at[global_start].set(jnp.arange(patches, dtype=jnp.int32), mode='drop')
    owner_patch = lax.cummax(start_marks, axis=0)
    segment = jnp.where(owner_patch >= 0, owner_patch, patches).astype(jnp.int32)
    projected = jnp.dot(states, weight, preferred_element_type=jnp.float32).astype(jnp.bfloat16)
    key_rows = projected[:, :key_width].astype(jnp.float32).reshape(length, HEADS, HD)
    value_rows = projected[:, key_width:].astype(jnp.float32).reshape(length, HEADS, HD)
    zero_row = jnp.zeros((1, key_width), jnp.bfloat16)
    query_rows = jnp.concatenate([queries, zero_row], 0)[segment].astype(jnp.float32).reshape(length, HEADS, HD)
    upstream = jnp.concatenate([grads_out, zero_row], 0)[segment].astype(jnp.float32).reshape(length, HEADS, HD)
    scores = lax.optimization_barrier(jnp.sum(query_rows * key_rows, -1)) * attn_scale
    row_peak = jax.ops.segment_max(scores, segment, num_segments=patches + 1)
    exponent = jnp.exp(scores - row_peak[segment])
    denominator = jax.ops.segment_sum(exponent, segment, num_segments=patches + 1)
    probabilities = exponent / denominator[segment]
    prob_half = lax.optimization_barrier(probabilities.astype(jnp.bfloat16)).astype(jnp.float32)
    prob_grad = lax.optimization_barrier(jnp.sum(upstream * value_rows, -1))
    delta_sum = jax.ops.segment_sum(probabilities * prob_grad, segment, num_segments=patches + 1)
    score_grad = (probabilities * (prob_grad - delta_sum[segment]) * attn_scale).astype(jnp.bfloat16)
    score_grad = lax.optimization_barrier(score_grad).astype(jnp.float32)
    weighted_keys = (score_grad[..., None] * key_rows).reshape(length, key_width)
    query_grad = jax.ops.segment_sum(weighted_keys, segment, num_segments=patches + 1)[:patches]
    query_grad = (loss_scale * query_grad).astype(jnp.bfloat16)
    key_grad = (loss_scale * score_grad[..., None] * query_rows).reshape(length, key_width)
    value_grad = (loss_scale * prob_half[..., None] * upstream).reshape(length, key_width)
    proj_grad = jnp.concatenate([key_grad, value_grad], 1).astype(jnp.bfloat16)
    byte_grad = jnp.dot(proj_grad, weight.T, preferred_element_type=jnp.float32).astype(jnp.bfloat16)
    weight_term = jnp.dot(states.T, proj_grad, preferred_element_type=jnp.float32)
    return (byte_grad, query_grad, weight_term)

def reference(byte_states, kv_weight, patch_query, out_grad, patch_start, patch_count):
    live_total = jnp.sum(patch_count.astype(jnp.float32))
    loss_scale = jnp.float32(SEQS * N_SEQ * PSLOT) / live_total

    def accumulate(running, per_seq):
        states, queries, grads_out, starts, counts = per_seq
        byte_grad, query_grad, weight_term = one_sequence(kv_weight, states, queries, grads_out, starts, counts, loss_scale)
        return (running + weight_term, (byte_grad, query_grad))
    initial = jnp.zeros((D, 2 * HEADS * HD), jnp.float32)
    kv_grad, (byte_grad, query_grad) = lax.scan(accumulate, initial, (byte_states, patch_query, out_grad, patch_start, patch_count))
    return (byte_grad, query_grad, kv_grad)
```

```python
import functools
import math

import jax
import jax.numpy as jnp
from jax import lax
from jax.experimental import pallas as pl
from jax.experimental.pallas import tpu as pltpu
from jax.sharding import PartitionSpec as P

HEADS = 8
HD = 64
PSLOT = 64
REACH = 64


def from_behind(value, axis, steps):
    count = lax.axis_size(axis)
    initial, last = (max(0, -steps), min(count, count - steps))
    return lax.ppermute(value, axis, [(source, source + steps) for source in range(initial, last)])


def plain_body(byte_states, kv_weight, patch_query, out_grad, patch_start, patch_count):
    seq_here, own_bytes, model_width = byte_states.shape
    half_width = patch_query.shape[2]
    shards = lax.axis_size("seq")
    position = lax.axis_index("seq")
    attn_scale = 1.0 / math.sqrt(HD)
    highest = lax.Precision.HIGHEST
    weight = lax.all_gather(kv_weight, "dp", axis=0, tiled=True)
    counts_here = lax.dynamic_slice_in_dim(patch_count, position, 1, 1)[:, 0]
    live_total = lax.psum(jnp.sum(counts_here.astype(jnp.float32)), ("dp", "seq"))
    loss_scale = jnp.float32(seq_here * lax.axis_size("dp") * shards * PSLOT) / live_total
    borrowed = from_behind(byte_states[:, :REACH], "seq", -1)
    extended = jnp.concatenate([byte_states, borrowed], 1)
    ext_rows = extended.shape[1]
    flat_states = extended.reshape(seq_here * ext_rows, model_width)
    projected = jnp.dot(flat_states, weight, preferred_element_type=jnp.float32).astype(
        jnp.bfloat16
    )
    projected = projected.reshape(seq_here, ext_rows, 2 * half_width)
    key_rows = (
        projected[..., :half_width].reshape(seq_here, ext_rows, HEADS, HD).astype(jnp.float32)
    )
    value_rows = (
        projected[..., half_width:].reshape(seq_here, ext_rows, HEADS, HD).astype(jnp.float32)
    )
    starts_here = lax.dynamic_slice_in_dim(patch_start, position, 1, 1)[:, 0, :]
    next_shard = jnp.minimum(position + 1, shards - 1)
    next_first = lax.dynamic_slice_in_dim(patch_start, next_shard, 1, 1)[:, 0, 0]
    final_end = jnp.where(position < shards - 1, own_bytes + next_first, own_bytes)
    slot_ids = jnp.arange(PSLOT, dtype=jnp.int32)
    shifted = jnp.concatenate([starts_here[:, 1:], starts_here[:, :1]], 1)
    patch_end = jnp.where(slot_ids[None, :] + 1 < counts_here[:, None], shifted, final_end[:, None])
    live_slots = slot_ids[None, :] < counts_here[:, None]
    byte_pos = jnp.arange(ext_rows, dtype=jnp.int32)
    member = (
        (byte_pos[None, :, None] >= starts_here[:, None, :])
        & (byte_pos[None, :, None] < patch_end[:, None, :])
        & live_slots[:, None, :]
    )
    inside = jnp.any(member, axis=2)
    onehot = member.astype(jnp.bfloat16)
    onehot_float = member.astype(jnp.float32)
    paired = jnp.concatenate([patch_query, out_grad], 2)
    spread = jnp.einsum("stp,spc->stc", onehot, paired, preferred_element_type=jnp.float32)
    query_rows = spread[..., :half_width].reshape(seq_here, ext_rows, HEADS, HD)
    upstream = spread[..., half_width:].reshape(seq_here, ext_rows, HEADS, HD)
    scores = jnp.sum(query_rows * key_rows, -1) * attn_scale
    masked = jnp.where(member[..., None], scores[:, :, None, :], -jnp.inf)
    row_peak = jnp.where(live_slots[..., None], jnp.max(masked, axis=1), 0.0)
    peak_rows = jnp.einsum("stp,sph->sth", onehot_float, row_peak, precision=highest)
    exponent = jnp.where(inside[..., None], jnp.exp(scores - peak_rows), 0.0)
    denominator = jnp.einsum("stp,sth->sph", onehot_float, exponent, precision=highest)
    denominator = jnp.where(live_slots[..., None], denominator, 1.0)
    denom_rows = jnp.einsum("stp,sph->sth", onehot_float, denominator, precision=highest)
    denom_rows = jnp.where(inside[..., None], denom_rows, 1.0)
    probabilities = exponent / denom_rows
    prob_half = lax.optimization_barrier(probabilities.astype(jnp.bfloat16)).astype(jnp.float32)
    prob_grad = jnp.sum(upstream * value_rows, -1)
    delta_sum = jnp.einsum(
        "stp,sth->sph", onehot_float, probabilities * prob_grad, precision=highest
    )
    delta_rows = jnp.einsum("stp,sph->sth", onehot_float, delta_sum, precision=highest)
    score_grad = (probabilities * (prob_grad - delta_rows) * attn_scale).astype(jnp.bfloat16)
    score_grad = lax.optimization_barrier(score_grad).astype(jnp.float32)
    weighted_keys = (score_grad[..., None] * key_rows).reshape(seq_here, ext_rows, half_width)
    query_grad = jnp.einsum("stp,stc->spc", onehot_float, weighted_keys, precision=highest)
    query_grad = (loss_scale * query_grad).astype(jnp.bfloat16)
    key_grad = (loss_scale * score_grad[..., None] * query_rows).reshape(
        seq_here, ext_rows, half_width
    )
    value_grad = (loss_scale * prob_half[..., None] * upstream).reshape(
        seq_here, ext_rows, half_width
    )
    proj_grad = jnp.concatenate([key_grad, value_grad], 2).astype(jnp.bfloat16)
    flat_grads = proj_grad.reshape(seq_here * ext_rows, 2 * half_width)
    state_grad = lax.dot_general(
        flat_grads, weight, (((1,), (1,)), ((), ())), preferred_element_type=jnp.float32
    )
    state_grad = state_grad.reshape(seq_here, ext_rows, model_width)
    outgoing = state_grad[:, own_bytes:].astype(jnp.bfloat16)
    handed = from_behind(outgoing, "seq", 1)
    rim_rows = handed.shape[1]
    local_part = state_grad[:, :own_bytes].at[:, :rim_rows].add(handed.astype(jnp.float32))
    byte_grad = local_part.astype(jnp.bfloat16)
    partial_value = lax.psum_scatter(
        lax.dot_general(
            flat_grads, flat_states, (((0,), (0,)), ((), ())), preferred_element_type=jnp.float32
        ),
        "seq",
        scatter_dimension=0,
        tiled=True,
    )
    partial_value = lax.psum_scatter(partial_value, "dp", scatter_dimension=1, tiled=True)
    kv_grad = partial_value.T
    return (byte_grad, query_grad, kv_grad)


NY = 2
CORES = 2
MESH = pl.DeviceIdType.MESH


def places():
    dp = lax.axis_index("dp")
    seq = lax.axis_index("seq")
    return (dp // NY, dp % NY, seq // CORES, seq % CORES)


def remote(src, dst, send, recv, dp, seq):
    return pltpu.make_async_remote_copy(
        src_ref=src,
        dst_ref=dst,
        send_sem=send,
        recv_sem=recv,
        device_id=(dp, seq),
        device_id_type=MESH,
    )


def flipped(value, mask):
    bit = 1
    while bit <= mask:
        if mask & bit:
            value = value + bit * (1 - 2 * ((value // bit) % 2))
        bit *= 2
    return value


def meet(n_dp, n_seq):
    dp = lax.axis_index("dp")
    seq = lax.axis_index("seq")
    z, y, x, c = places()
    n_z = n_dp // NY
    barrier = pltpu.get_barrier_semaphore()
    for step in range(1, n_dp):
        pl.semaphore_signal(
            barrier, inc=1, device_id=(lax.rem(dp + step, n_dp), seq), device_id_type=MESH
        )
    for step in range(1, n_seq):
        pl.semaphore_signal(
            barrier, inc=1, device_id=(dp, lax.rem(seq + step, n_seq)), device_id_type=MESH
        )
    for mask in range(1, n_z):
        pl.semaphore_signal(
            barrier,
            inc=1,
            device_id=(flipped(z, mask) * NY + y, x * CORES + 1 - c),
            device_id_type=MESH,
        )
    pl.semaphore_wait(barrier, n_dp - 1 + n_seq - 1 + n_z - 1)


def whole_kernel(
    n_dp, n_seq, slots_all,
    w_ref, ps_hbm, pc_hbm, states_ref, pq_hbm, og_hbm,
    byte_ref, qg_ref, out_ref,
    ps_ref, pc_ref, w_all, counts, cnt_src, ext, ext_t, proj, pgrad, split, pq_ref, og_ref,
    g_send, g_keep, g_buf, rim, handed,
    a_out, a_buf, hold, b_out, b_buf, z_out, z_buf, s_out, s_buf,
    l_sem, gz_send, gz_recv, gy_send, gy_recv, gx_send, gx_recv, gc_send, gc_recv,
    n_send, n_recv, h_send, h_recv,
    c_send, c_recv, a_send, a_recv, b_send, b_recv, z_send, z_recv, s_send, s_recv, r_send, r_recv,
):
    z, y, x, c = places()
    n_z = n_dp // NY
    me_dp, me_seq = lax.axis_index("dp"), lax.axis_index("seq")
    x_peer, c_peer = (1 - x) * CORES + c, x * CORES + 1 - c
    y_peer = z * NY + 1 - y
    q_own, q_core = x + CORES * c, x + CORES * (1 - c)
    q_over, q_far = 1 - x + CORES * c, 1 - x + CORES * (1 - c)
    rows, model = w_ref.shape
    width = w_ref.shape[1] // n_seq
    own_bytes = states_ref.shape[0]
    reach = rim.shape[0]

    def rows_of(block):
        return pl.ds(pl.multiple_of(block * rows, rows), rows)

    def cols_of(quarter):
        return pl.ds(pl.multiple_of(quarter * width, width), width)

    loads = [
        pltpu.make_async_copy(states_ref, ext.at[pl.ds(0, own_bytes)], l_sem.at[0]),
        pltpu.make_async_copy(pq_hbm, pq_ref, l_sem.at[1]),
        pltpu.make_async_copy(og_hbm, og_ref, l_sem.at[2]),
        pltpu.make_async_copy(w_ref, w_all.at[rows_of(me_dp)], l_sem.at[3]),
        pltpu.make_async_copy(pc_hbm, pc_ref, l_sem.at[4]),
        pltpu.make_async_copy(ps_hbm, ps_ref, l_sem.at[5]),
    ]
    for k in (4, 3, 0, 1, 2, 5):
        loads[k].start()
    loads[4].wait()
    total = pc_ref[0, 0]
    for shard in range(1, n_seq):
        total = total + pc_ref[0, shard]
    cnt_src[...] = jnp.full(cnt_src.shape, total.astype(jnp.float32))
    counts[0] = cnt_src[...]
    meet(n_dp, n_seq)
    loads[3].wait()

    def part(block, quarter):
        return w_all.at[rows_of(block), cols_of(quarter)]

    def block_of(d, other):
        return lax.rem(z + d, n_z) * NY + (1 - y if other else y)

    started = []

    def go(copy):
        copy.start()
        started.append(copy)

    def arrived(dst, send, recv):
        remote(dst, dst, send, recv, me_dp, x_peer).wait_recv()

    z_order = [1, n_z - 1] + list(range(2, n_z - 1)) if n_z > 2 else list(range(1, n_z))
    if n_z == 4:
        targets = [z + 1 - 2 * lax.rem(z, 2), jnp.where(z < 2, 2, 1), jnp.where(z < 2, 3, 0)]
    else:
        targets = [lax.rem(z + d, n_z) for d in z_order]
    ahead = [lax.rem(t - z + n_z, n_z) for t in targets]
    behind = [lax.rem(z - t + n_z, n_z) for t in targets]
    own = part(me_dp, q_own)
    for t, d in zip(targets, ahead):
        go(remote(own, own, gz_send.at[d], gz_recv.at[d], t * NY + y, me_seq))
    for side, column in enumerate((q_own, q_over)):
        piece = part(me_dp, column)
        go(
            remote(
                piece, piece, gy_send.at[side * n_z], gy_recv.at[side * n_z], y_peer, me_seq
            )
        )
    loads[0].wait()

    @pl.when(me_seq > 0)
    def _():
        remote(
            ext.at[pl.ds(0, reach)], ext.at[pl.ds(own_bytes, reach)], h_send, h_recv,
            me_dp, me_seq - 1,
        ).start()

    @pl.when(me_seq == n_seq - 1)
    def _():
        ext[own_bytes:, :] = jnp.zeros((reach, model), ext.dtype)

    for step in range(1, n_dp):
        go(
            remote(
                cnt_src, counts.at[step], n_send.at[step], n_recv.at[step],
                lax.rem(me_dp + step, n_dp), me_seq,
            )
        )

    ext_t[:, :own_bytes] = ext[:own_bytes, :].T

    def back_block(d, other):
        return block_of(n_z - d, other)

    def share(d, other, over=True):
        here = part(back_block(d, other), q_own)
        slot = n_z * other + d
        if over:
            go(remote(here, here, gx_send.at[slot], gx_recv.at[slot], me_dp, x_peer))
        go(remote(here, here, gc_send.at[0, slot], gc_recv.at[0, slot], me_dp, c_peer))

    for k, d in enumerate(behind):
        here = part(back_block(d, 0), q_own)
        arrived(here, gz_send.at[d], gz_recv.at[d])
        go(remote(here, here, gy_send.at[d], gy_recv.at[d], y_peer, me_seq))
        share(d, 0)
    arrived(part(y_peer, q_own), gy_send.at[0], gy_recv.at[0])
    share(0, 1, False)
    there = part(y_peer, q_over)
    arrived(there, gy_send.at[n_z], gy_recv.at[n_z])
    go(remote(there, there, gc_send.at[1, n_z], gc_recv.at[1, n_z], me_dp, c_peer))
    for d in behind:
        arrived(part(back_block(d, 1), q_own), gy_send.at[d], gy_recv.at[d])
        share(d, 1)

    @pl.when(me_seq < n_seq - 1)
    def _():
        arrived(ext.at[pl.ds(own_bytes, reach)], h_send, h_recv)

    pos = me_seq
    shards = n_seq
    ext_rows = ext.shape[0]
    key_width = pq_ref.shape[1]
    half = width // 2
    attn_scale = 1.0 / math.sqrt(HD)
    tile = 256
    last = (((1,), (1,)), ((), ()))
    first = (((0,), (0,)), ((), ()))

    def project(quarter):
        cols = cols_of(quarter)
        proj[:, cols] = jnp.dot(
            ext[...], w_all[:, cols], preferred_element_type=jnp.float32
        ).astype(jnp.bfloat16)

    order = [(d, other) for other in (0, 1) for d in behind]
    project(q_own)
    ext_t[:, own_bytes:] = ext[own_bytes:, :].T
    for step in range(1, n_dp):
        arrived(counts.at[step], n_send.at[step], n_recv.at[step])
    for k in (1, 2, 5):
        loads[k].wait()
    loss_scale = slots_all / jnp.sum(counts[...], axis=0)[0:1, 0:1]

    count = pc_ref[0, pos]
    starts = ps_ref[pl.ds(pos, 1), :]
    nxt = jnp.minimum(pos + 1, shards - 1)
    next_first = ps_ref[pl.ds(nxt, 1), :][:, 0:1]
    final_end = jnp.where(pos < shards - 1, own_bytes + next_first, own_bytes)
    shifted = jnp.concatenate([starts[:, 1:], starts[:, :1]], 1)
    slot_ids = lax.broadcasted_iota(jnp.int32, (1, PSLOT), 1)
    ends = jnp.where(slot_ids + 1 < count, shifted, final_end)
    ends = jnp.where(slot_ids < count, ends, 0)
    heads = width // HD
    slots = heads * PSLOT
    starts = jnp.concatenate([starts] * heads, 1)
    ends = jnp.concatenate([ends] * heads, 1)
    byte_pos = lax.broadcasted_iota(jnp.int32, (ext_rows, slots), 0)
    member = (byte_pos >= starts) & (byte_pos < ends)
    same = (lax.broadcasted_iota(jnp.int32, (slots, width), 0) // PSLOT) == (
        lax.broadcasted_iota(jnp.int32, (slots, width), 1) // HD
    )

    def diag(block):
        every = jnp.concatenate([block] * heads, 0).astype(jnp.float32)
        return jnp.where(same, every, 0.0).astype(jnp.bfloat16)

    def lanes(index):
        return pl.ds(pl.multiple_of(index * half, half), half)

    def divide(stage, kind, value):
        for side in (0, 1):
            place = 2 * (1 - c - side + 2 * c * side) + kind + x - 2 * kind * x
            split[stage, :, lanes(place)] = value[:, side * half : (side + 1) * half]

    def attend(stage, group):
        kc, vc = cols_of(group), cols_of(group + CORES)
        query = diag(pq_ref[:, kc])
        up = diag(og_ref[:, kc])
        keys = proj[:, kc]
        score = lax.dot_general(keys, query, last, preferred_element_type=jnp.float32)
        score = jnp.where(member, score * attn_scale, -1e30)
        peak = jnp.max(score, axis=0, keepdims=True)
        expo = jnp.where(member, jnp.exp(score - peak), 0.0)
        denom = jnp.sum(expo, axis=0, keepdims=True)
        prob = expo / jnp.where(denom > 0.0, denom, 1.0)
        prob_grad = lax.dot_general(proj[:, vc], up, last, preferred_element_type=jnp.float32)
        delta = jnp.sum(prob * prob_grad, axis=0, keepdims=True)
        score_grad = (prob * (prob_grad - delta) * attn_scale).astype(jnp.bfloat16)
        key_grad = (
            loss_scale * jnp.dot(score_grad, query, preferred_element_type=jnp.float32)
        ).astype(jnp.bfloat16)
        value_grad = (
            loss_scale
            * jnp.dot(prob.astype(jnp.bfloat16), up, preferred_element_type=jnp.float32)
        ).astype(jnp.bfloat16)
        pgrad[:, kc] = key_grad
        pgrad[:, vc] = value_grad
        divide(stage, 0, key_grad)
        divide(stage, 1, value_grad)
        qg = lax.dot_general(score_grad, keys, first, preferred_element_type=jnp.float32)
        qg = jnp.where(same, qg, 0.0)
        qg = sum(qg[h * PSLOT : (h + 1) * PSLOT] for h in range(heads))
        qg_ref[:, kc] = (loss_scale * qg).astype(jnp.bfloat16)

    masks = [mask for mask in (2, 3) if mask < n_z] + [1] if n_z > 1 else []
    masks = masks + list(range(4, n_z)) + [0]
    both = NY * rows

    def rows_at(mask):
        return pl.ds(pl.multiple_of(flipped(z, mask) * both, both), both)

    def weight_terms(stage):
        g_send[stage] = jnp.dot(
            ext_t[...], split[stage, :, :width], preferred_element_type=jnp.float32
        ).astype(jnp.bfloat16)
        for mask in masks:
            there = rows_at(mask)
            go(
                remote(
                    g_send.at[stage, there], g_buf.at[stage, there],
                    c_send.at[stage, mask], c_recv.at[stage, mask], me_dp, c_peer,
                )
            )
        g_keep[stage] = jnp.dot(
            ext_t[...], split[stage, :, width:], preferred_element_type=jnp.float32
        )

    a_dev = (me_dp * (1 - c) + y_peer * c, x_peer * (1 - c) + me_seq * c)
    b_dev = (y_peer * (1 - c) + me_dp * c, me_seq * (1 - c) + x_peer * c)

    def paired(stage, mask, one, two):
        across, other = one * (1 - c) + two * c, one * c + two * (1 - c)
        here = rows_of(flipped(z, mask) * NY + y + other * (1 - 2 * y))
        cols = lanes(across)
        return g_keep[stage, here, cols] + g_buf[stage, here, cols].astype(jnp.float32)

    def step_a(stage):
        twin = stage * c + (1 - stage) * (1 - c)
        for mask in masks:
            there = g_buf.at[stage, rows_at(mask)]
            arrived(there, c_send.at[stage, mask], c_recv.at[stage, mask])
            for two in (0, 1):
                a_out[stage, mask, two * rows : (two + 1) * rows] = paired(
                    stage, mask, 1, two
                ).astype(jnp.bfloat16)
            go(
                remote(
                    a_out.at[stage, mask], a_buf.at[twin, mask],
                    a_send.at[stage, mask], a_recv.at[twin, mask], *a_dev,
                )
            )

    def step_b(stage):
        twin = stage * (1 - c) + (1 - stage) * c
        for mask in masks:
            arrived(a_buf.at[stage, mask], a_send.at[stage, mask], a_recv.at[stage, mask])
            b_out[stage, mask] = (
                paired(stage, mask, 0, 1) + a_buf[stage, mask, rows:].astype(jnp.float32)
            ).astype(jnp.bfloat16)
            go(
                remote(
                    b_out.at[stage, mask], b_buf.at[twin, mask],
                    b_send.at[stage, mask], b_recv.at[twin, mask], *b_dev,
                )
            )
            hold[stage, mask] = paired(stage, mask, 0, 0) + a_buf[stage, mask, :rows].astype(
                jnp.float32
            )

    def step_z(stage, group):
        for mask in masks:
            arrived(b_buf.at[stage, mask], b_send.at[stage, mask], b_recv.at[stage, mask])
            value = hold[stage, mask] + b_buf[stage, mask].astype(jnp.float32)
            if mask:
                z_out[stage, mask] = value.astype(jnp.bfloat16)
                go(
                    remote(
                        z_out.at[stage, mask], z_buf.at[c, mask],
                        z_send.at[stage, mask], z_recv.at[c, mask],
                        flipped(z, mask) * NY + y, x * CORES + group,
                    )
                )
                continue

            @pl.when(c == group)
            def _():
                out_ref[:, lanes(c)] = value

            @pl.when(c != group)
            def _():
                s_out[...] = value.astype(jnp.bfloat16)
                remote(s_out, s_buf, s_send, s_recv, me_dp, c_peer).start()

    def back(lo, hi):
        @pl.loop(lo, hi)
        def _(n):
            cols = pl.ds(pl.multiple_of(n * tile, tile), tile)
            value = lax.dot_general(
                pgrad[...], w_all[cols, :], last, preferred_element_type=jnp.float32
            ).astype(jnp.bfloat16)
            byte_ref[:, cols] = value[:own_bytes]
            rim[:, cols] = value[own_bytes:]

    for d, other in [(0, 1)] + order:
        slot = n_z * other + d
        arrived(part(back_block(d, other), q_core), gc_send.at[0, slot], gc_recv.at[0, slot])
    project(q_core)
    attend(0, x)
    weight_terms(0)
    for d, other in order:
        slot = n_z * other + d
        piece = part(back_block(d, other), q_over)
        arrived(piece, gx_send.at[slot], gx_recv.at[slot])
        go(remote(piece, piece, gc_send.at[1, slot], gc_recv.at[1, slot], me_dp, c_peer))
    step_a(0)
    project(q_over)
    for d, other in [(0, 1)] + order:
        slot = n_z * other + d
        arrived(part(back_block(d, other), q_far), gc_send.at[1, slot], gc_recv.at[1, slot])
    project(q_far)
    attend(1, 1 - x)
    weight_terms(1)
    step_a(1)
    step_b(1 - c)
    back(0, model // tile)

    @pl.when(me_seq < n_seq - 1)
    def _():
        remote(rim, handed, r_send, r_recv, me_dp, me_seq + 1).start()

    step_b(c)
    step_z(1, 1 - x)
    step_z(0, x)

    @pl.when(me_seq > 0)
    def _():
        arrived(handed, r_send, r_recv)
        byte_ref[:reach, :] = (
            byte_ref[:reach, :].astype(jnp.float32) + handed[...].astype(jnp.float32)
        ).astype(jnp.bfloat16)

    arrived(s_buf, s_send, s_recv)
    for side, core in enumerate((c, 1 - c)):
        done = s_buf[...].astype(jnp.float32) if side else out_ref[:, lanes(c)]
        for mask in masks[:-1]:
            arrived(z_buf.at[core, mask], z_send.at[0, mask], z_recv.at[core, mask])
            done = done + z_buf[core, mask].astype(jnp.float32)
        out_ref[:, lanes(core)] = done
    remote(s_out, s_buf, s_send, s_recv, me_dp, c_peer).wait_send()

    @pl.when(me_seq > 0)
    def _():
        remote(
            ext.at[pl.ds(0, reach)], ext.at[pl.ds(own_bytes, reach)], h_send, h_recv,
            me_dp, me_seq - 1,
        ).wait_send()

    @pl.when(me_seq < n_seq - 1)
    def _():
        remote(rim, handed, r_send, r_recv, me_dp, me_seq + 1).wait_send()

    for copy in started:
        copy.wait_send()


def hand_out(a_in, b_in, c_in, a_out, b_out, c_out, sem):
    copies = [
        pltpu.make_async_copy(src, dst, sem.at[k])
        for k, (src, dst) in enumerate(((a_in, a_out), (b_in, b_out), (c_in, c_out)))
    ]
    for copy in copies:
        copy.start()
    for copy in copies:
        copy.wait()


def kernel_body(byte_states, kv_weight, patch_query, out_grad, patch_start, patch_count):
    n_dp, n_seq = lax.axis_size("dp"), lax.axis_size("seq")
    n_z = n_dp // NY
    model = byte_states.shape[2]
    own_bytes = byte_states.shape[1]
    rows, cols = kv_weight.shape
    width = cols // n_seq
    key_width = patch_query.shape[2]
    ext_rows = own_bytes + REACH
    vmem = pl.BlockSpec(memory_space=pltpu.VMEM)
    hbm = pl.BlockSpec(memory_space=pltpu.HBM)
    half = jnp.bfloat16

    def buf(*shape, dtype=half):
        return pltpu.VMEM(shape, dtype)

    def sems(*shape):
        return [pltpu.SemaphoreType.DMA(shape)] * 2

    byte_grad, query_grad, kv_grad = pl.pallas_call(
        functools.partial(whole_kernel, n_dp, n_seq, float(n_dp * n_seq * PSLOT)),
        out_shape=(
            pltpu.VMEM((own_bytes, model), half),
            pltpu.VMEM((PSLOT, key_width), half),
            pltpu.VMEM((rows, width), jnp.float32),
        ),
        in_specs=[hbm] * 6,
        out_specs=(vmem, vmem, vmem),
        scratch_shapes=[
            pltpu.VMEM(patch_start.shape[1:], jnp.int32),
            pltpu.SMEM(patch_count.shape, jnp.int32),
            buf(model, cols),
            buf(n_dp, 8, 128, dtype=jnp.float32),
            buf(8, 128, dtype=jnp.float32),
            buf(ext_rows, model),
            buf(model, ext_rows),
            buf(ext_rows, cols),
            buf(ext_rows, cols),
            buf(2, ext_rows, 2 * width),
            buf(PSLOT, key_width),
            buf(PSLOT, key_width),
            buf(2, model, width),
            buf(2, model, width, dtype=jnp.float32),
            buf(2, model, width),
            buf(REACH, model),
            buf(REACH, model),
            buf(2, n_z, NY * rows, width // 2),
            buf(2, n_z, NY * rows, width // 2),
            buf(2, n_z, rows, width // 2, dtype=jnp.float32),
            buf(2, n_z, rows, width // 2),
            buf(2, n_z, rows, width // 2),
            buf(2, n_z, rows, width // 2),
            buf(2, n_z, rows, width // 2),
            buf(rows, width // 2),
            buf(rows, width // 2),
            pltpu.SemaphoreType.DMA((6,)),
            *sems(n_z), *sems(2 * n_z), *sems(n_dp), *sems(2, n_dp),
            *sems(n_dp), *sems(),
            *sems(2, n_z), *sems(2, n_z), *sems(2, n_z), *sems(2, n_z), *sems(), *sems(),
        ],
        compiler_params=pltpu.CompilerParams(
            collective_id=0, has_side_effects=True, vmem_limit_bytes=63 * 1024 * 1024
        ),
        name="whole",
    )(
        kv_weight, patch_start[0], patch_count, byte_states[0], patch_query[0], out_grad[0]
    )
    byte_grad, query_grad, kv_grad = pl.pallas_call(
        hand_out,
        out_shape=(
            jax.ShapeDtypeStruct((own_bytes, model), half),
            jax.ShapeDtypeStruct((PSLOT, key_width), half),
            jax.ShapeDtypeStruct((rows, width), jnp.float32),
        ),
        in_specs=[pl.BlockSpec(memory_space=pl.ANY)] * 3,
        out_specs=[hbm] * 3,
        scratch_shapes=[pltpu.SemaphoreType.DMA((3,))],
        compiler_params=pltpu.CompilerParams(vmem_limit_bytes=1024 * 1024),
        name="hand_out",
    )(byte_grad, query_grad, kv_grad)
    return (byte_grad[None], query_grad[None], kv_grad)


def body(byte_states, kv_weight, patch_query, out_grad, patch_start, patch_count):
    n_dp, n_seq = lax.axis_size("dp"), lax.axis_size("seq")
    fits = (
        n_seq == 2 * CORES
        and n_dp % NY == 0
        and n_dp <= 16
        and byte_states.shape[0] == 1
        and n_dp // NY in (2, 4, 8)
        and kv_weight.shape[1] % (256 * n_seq) == 0
        and kv_weight.shape[1] == 2 * patch_query.shape[2]
    )
    chosen = kernel_body if fits else plain_body
    return chosen(byte_states, kv_weight, patch_query, out_grad, patch_start, patch_count)


def solution(mesh):
    in_specs = (
        P("dp", "seq", None),
        P("dp", None),
        P("dp", "seq", None),
        P("dp", "seq", None),
        P("dp", None, None),
        P("dp", None),
    )
    out_specs = (P("dp", "seq", None), P("dp", "seq", None), P("dp", "seq"))
    return jax.shard_map(body, mesh=mesh, in_specs=in_specs, out_specs=out_specs, check_vma=False)
```
